128 devices in a mesh: sub: 128 (over y, z, x, core).
Axes of the slice: x: 4, y: 4, z: 4, core: 2. Of those that a mesh axis runs over, the one named last changes fastest.
Arguments:
- right_side: float32 [512, 128, 512], P('sub'), may hold values from -8 to 8
- sigma: float32 [512, 128, 512], P('sub'), may hold values from 0.25 to 2
- wind: float32 [512, 128, 512], P('sub'), may hold values from -0.8 to 0.8
- local_inverse: float32 [128, 512, 512], P('sub'), may hold values from -1 to 2, as said below
- basis_y: float32 [128, 32], replicated, may hold values from -0.5 to 0.5
- basis_z: float32 [512, 64], replicated, may hold values from -0.25 to 0.25
- gamma: float32 [7, 32, 64], replicated, may hold values from 0.3 to 3
Outputs:
- solution_field: float32 [512, 128, 512], P('sub')
- residual: float32 [512, 128, 512], P('sub')
The draws below stay inside these ranges and needn't reach their ends.
Inputs may be any that keep to these rules, and one draw needn't show every extreme that they name: `local_inverse`: each block is the identity plus a perturbation whose entries lie within 2/sqrt(512) of zero; each row of the perturbation has norm about one half.
All inputs are finite; a program needn't handle non-finite values.
Results may differ from the reference program's by a relative error of at most 0.00022.
Values sent between devices are 32-bit elements; how exact they have to be, the bound alone decides.
A program may use at most 64 MiB of HBM per device.

```python
import math
import jax
import jax.numpy as jnp
from jax import lax

CX = 4
NY = 128
NZ = 512
KY = 32
KZ = 64
BLOCKS = 128
NX = 512
LEVELS = 7
N_SUB = 128


def draw_local_inverse(key, part):
    noise = jnp.clip(jax.random.normal(key, (BLOCKS, NZ, NZ), jnp.float32), -4.0, 4.0)
    scaled = noise * (0.5 / jnp.sqrt(jnp.float32(NZ)))
    return scaled + jnp.eye(NZ, dtype=jnp.float32)[None]


def block_scale(own_key, shape, split, low, top_value):
    def one(axis_at, shards_of):
        steps = jax.random.uniform(jax.random.fold_in(jax.random.fold_in(own_key, 6), axis_at), (shards_of,), jnp.float32, low / len(split), top_value / len(split))
        return jnp.repeat(jnp.exp(steps), shape[axis_at] // shards_of).reshape((-1,) + (1,) * (len(shape) - axis_at - 1))

    gain = one(*split[0])
    for cut in split[1:]:
        gain = gain * one(*cut)
    return gain


def bell_draw(key, extent, deviation, reach, pieces=(), held_as=jnp.bfloat16):
    loudness = block_scale(key, extent, pieces, -0.22, 0.18) if pieces else 1.0
    result = jax.random.normal(key, extent, jnp.float32) * deviation * loudness
    return jnp.minimum(jnp.maximum(result, -reach), reach).astype(held_as)


def setup_inputs(seed: int = 0) -> dict:
    key_list = jax.random.split(jax.random.key(seed), 8)
    return {
        "right_side": bell_draw(key_list[0], (NX, NY, NZ), 1.0, 8.0, ((0, 128),), jnp.float32),
        "sigma": jnp.clip(0.25 + 1.75 * jax.random.uniform(key_list[1], (NX, NY, NZ), jnp.float32) ** block_scale(key_list[1], (NX, NY, NZ), ((0, 128),), -0.2, 0.2), 0.25, 2.0),
        "wind": jnp.clip(jax.random.uniform(key_list[2], (NX, NY, NZ), jnp.float32, -0.8, 0.8) * block_scale(key_list[2], (NX, NY, NZ), ((0, 128),), -0.4, 0.0), -0.8, 0.8),
        "local_inverse": draw_local_inverse(jax.random.fold_in(key_list[7], 71), 0),
        "basis_y": bell_draw(key_list[4], (NY, KY), NY ** -0.5, 0.5, (), jnp.float32),
        "basis_z": bell_draw(key_list[5], (NZ, KZ), NZ ** -0.5, 0.25, (), jnp.float32),
        "gamma": jnp.clip(jnp.exp(jax.random.uniform(key_list[6], (LEVELS, KY, KZ), jnp.float32, math.log(0.3), math.log(3.0))), 0.3, 3.0),
    }


HIGH = lax.Precision.HIGHEST

def apply_operator(field, sigma, wind):
    padded_x = jnp.pad(field, ((1, 1), (0, 0), (0, 0)))
    upper = padded_x[2:]
    lower = padded_x[:-2]
    padded_y = jnp.pad(field, ((0, 0), (1, 1), (0, 0)))
    padded_z = jnp.pad(field, ((0, 0), (0, 0), (1, 1)))
    beside = upper + lower + padded_y[:, 2:] + padded_y[:, :-2] + padded_z[:, :, 2:] + padded_z[:, :, :-2]
    return (6.0 + sigma) * field - beside + wind * (upper - lower)

def precondition(field, local_inverse, basis_y, basis_z, gamma):
    blocks = field.reshape(N_SUB, CX, NY, NZ)
    local = jnp.einsum('bxyz,bzw->bxyw', blocks, local_inverse, precision=HIGH)
    summed = lax.optimization_barrier(jnp.sum(blocks, axis=1))
    half = jnp.einsum('byz,zm->bym', summed, basis_z, precision=HIGH)
    proj = jnp.einsum('yk,bym->bkm', basis_y, half, precision=HIGH)
    coarse = jnp.zeros((N_SUB, KY, KZ), jnp.float32)
    for level in range(LEVELS):
        width = 2 ** (level + 1)
        grouped = lax.optimization_barrier(jnp.sum(proj.reshape(N_SUB // width, width, KY, KZ), axis=1, keepdims=True))
        grouped = jnp.broadcast_to(grouped, (N_SUB // width, width, KY, KZ)).reshape(N_SUB, KY, KZ)
        coarse = coarse + gamma[level] * grouped / jnp.sqrt(jnp.float32(CX * width))
    back = jnp.einsum('bkm,zm->bkz', coarse, basis_z, precision=HIGH)
    spread = jnp.einsum('yk,bkz->byz', basis_y, back, precision=HIGH)
    return (local + spread[:, None]).reshape(NX, NY, NZ)

def reference(right_side, sigma, wind, local_inverse, basis_y, basis_z, gamma):

    def inner(left, right):
        return jnp.sum(left * right)
    beta = jnp.sqrt(inner(right_side, right_side))
    first = right_side / beta
    z_one = precondition(first, local_inverse, basis_y, basis_z, gamma)
    image = apply_operator(z_one, sigma, wind)
    h11 = inner(first, image)
    image = image - h11 * first
    h21 = jnp.sqrt(inner(image, image))
    second = image / h21
    z_two = precondition(second, local_inverse, basis_y, basis_z, gamma)
    image = apply_operator(z_two, sigma, wind)
    h12 = inner(first, image)
    h22 = inner(second, image)
    image = image - h12 * first - h22 * second
    h32 = jnp.sqrt(inner(image, image))
    m11 = h11 * h11 + h21 * h21
    m12 = h11 * h12 + h21 * h22
    m22 = h12 * h12 + h22 * h22 + h32 * h32
    q_one = h11 * beta
    q_two = h12 * beta
    determ = m11 * m22 - m12 * m12
    y_one = (m22 * q_one - m12 * q_two) / determ
    y_two = (m11 * q_two - m12 * q_one) / determ
    solution_field = y_one * z_one + y_two * z_two
    residual = right_side - apply_operator(solution_field, sigma, wind)
    return (solution_field, residual)
```

```python
import functools

import jax
import jax.numpy as jnp
from jax import lax
from jax.experimental import pallas as pl
from jax.experimental.pallas import tpu as pltpu
from jax.sharding import PartitionSpec as P

MESH = pl.DeviceIdType.MESH
F32 = jnp.float32
BF16 = jnp.bfloat16

CX, NY, NZ, KY, KZ, LEVELS = 4, 128, 512, 32, 64, 7
PK = 16
PAY = PK + 8
TOP = 8
PADY = NY + 2 * TOP


def split(x):
    high = x.astype(BF16)
    return high, (x - high.astype(F32)).astype(BF16)


def dot(a, b):
    return jnp.dot(a, b, preferred_element_type=F32)


def dot3(a, b):
    ah, al = a
    bh, bl = b
    return dot(ah, bh) + dot(al, bh) + dot(ah, bl)


def lanes(shape):
    return lax.broadcasted_iota(jnp.int32, shape, len(shape) - 1)


def pack(c):
    return jnp.where(lanes((PK, 128)) < KZ, c[:PK], c[PK:])


def masked(c):
    low = lanes((PK, 128)) < KZ
    return jnp.concatenate([jnp.where(low, c, 0.0), jnp.where(low, 0.0, c)], axis=0)


def neighbours_z(c):
    lane = lanes(c.shape)
    ahead = jnp.where(lane == NZ - 1, 0.0, pltpu.roll(c, NZ - 1, 1))
    behind = jnp.where(lane == 0, 0.0, pltpu.roll(c, 1, 1))
    return ahead + behind


def total(x):
    return jnp.sum(jnp.sum(x, axis=0, keepdims=True), axis=1, keepdims=True)


def fold(x):
    acc = x[0:8]
    for i in range(8, x.shape[0], 8):
        acc = acc + x[i : i + 8]
    return acc


def fold_lanes(x):
    return x[:, 0:128] + x[:, 128:256] + x[:, 256:384] + x[:, 384:512]


def kernel(
    r_h, sg_h, wd_h, mi_h, by_h, bz_h, gm_h,
    sol, res,
    R, SG, WD, MI, BY, BZ, GM,
    XB, MH, ML, L, LW, AL, W, Q, Z1, U2,
    BZH, BZL, TBH, TBL, B2H, B2L, BYH, BYL, BY2H, BY2L, BTH, BTL, GP,
    S3, G0, X, CS, SUM, PL,
    SND, RCV, CP, NBC, SC,
    ld_sem, snd_sem, rcv_sem, cps_sem, cpr_sem, hs_sem, hr_sem,
):
    b = lax.axis_index("sub")
    core = lax.rem(b, 2)
    cx = lax.rem(b // 2, 4)
    cz = lax.rem(b // 8, 4)
    cy = b // 32
    coords = (cx, cz, cy)
    strides = (2, 8, 32)
    mate = b + 1 - 2 * core
    far = b - 1 + 2 * core
    has_far = jnp.logical_and(far >= 0, far < 128)

    def peer(axis, d):
        c = coords[axis]
        return b + (lax.rem(c + d, 4) - c) * strides[axis]

    loads = [
        pltpu.make_async_copy(src, dst, ld_sem.at[i])
        for i, (src, dst) in enumerate(
            [(r_h, R), (by_h, BY), (bz_h, BZ), (mi_h.at[0], MI), (gm_h, GM), (sg_h, SG), (wd_h, WD)]
        )
    ]
    for c in loads:
        c.start()

    barrier = pltpu.get_barrier_semaphore()
    peers = [mate] + [peer(a, d) for a in range(3) for d in (1, 2, 3)]
    for p in peers:
        pl.semaphore_signal(barrier, inc=1, device_id=(p,), device_id_type=MESH)

    @pl.when(has_far)
    def _():
        pl.semaphore_signal(barrier, inc=1, device_id=(far,), device_id_type=MESH)

    loads[1].wait()
    loads[2].wait()
    by = BY[...]
    bz = BZ[...]
    bz2 = jnp.concatenate([bz, bz], axis=1)
    B2H[...], B2L[...] = split(bz2)
    BTH[...], BTL[...] = split(by.T)

    def project(field):
        half = dot3(split(field), (B2H[...], B2L[...]))
        return pack(dot3((BTH[...], BTL[...]), split(half)))

    loads[0].wait()
    acc = jnp.zeros((8, NZ), F32)
    for y in range(0, NY, 16):
        s = jnp.zeros((16, NZ), F32)
        q = jnp.zeros((16, NZ), F32)
        for x in range(CX):
            v = R[x, y : y + 16]
            s = s + v
            q = q + v * v
        X[y : y + 16] = s
        acc = acc + fold(q)
    SND[0, 0, :PK] = project(X[...])
    SND[0, 0, PK:] = fold_lanes(acc)

    pl.semaphore_wait(barrier, len(peers) + has_far.astype(jnp.int32))

    sends = []

    def send(src, dst, ss, rs, device):
        c = pltpu.make_async_remote_copy(
            src_ref=src, dst_ref=dst, send_sem=ss, recv_sem=rs, device_id=(device,), device_id_type=MESH
        )
        c.start()
        return c

    def to_mate(k, rows):
        c = send(SND.at[k, 0, rows], RCV.at[k, 0, rows], snd_sem.at[k, 0], rcv_sem.at[k, 0], mate)
        sends.append(c)
        return c

    def to_axis(k, axis, rows):
        cs = []
        for d in (1, 2, 3):
            i = 1 + 3 * axis + d - 1
            cs.append(
                send(SND.at[k, 1 + axis, rows], RCV.at[k, i, rows], snd_sem.at[k, i], rcv_sem.at[k, i], peer(axis, d))
            )
        sends.extend(cs)
        return cs

    def axis_sums(k, axis, rows):
        base = 1 + 3 * axis
        odd = lax.rem(coords[axis], 2)
        own = SND[k, 1 + axis, rows] + RCV[k, base + 2 - 2 * odd, rows]
        other = RCV[k, base + 1, rows] + RCV[k, base + 2 * odd, rows]
        return own, other, own + other

    ALLR = pl.ds(0, PAY)
    PKR = pl.ds(0, PK)
    SCR = pl.ds(PK, 8)

    def edges(k, field):
        send_mate = send(
            field.at[4 - 3 * core, TOP : TOP + NY], field.at[5 * core, TOP : TOP + NY],
            hs_sem.at[k, 0], hr_sem.at[k, 0], mate,
        )
        sends.append(send_mate)

        @pl.when(has_far)
        def _():
            send(
                field.at[1 + 3 * core, TOP : TOP + NY], field.at[5 - 5 * core, TOP : TOP + NY],
                hs_sem.at[k, 1], hr_sem.at[k, 1], far,
            )

    def edge_copy(k, field):
        return pltpu.make_async_remote_copy(
            src_ref=field.at[1 + 3 * core, TOP : TOP + NY], dst_ref=field.at[5 - 5 * core, TOP : TOP + NY],
            send_sem=hs_sem.at[k, 1], recv_sem=hr_sem.at[k, 1], device_id=(far,), device_id_type=MESH,
        )

    def mate_edge(k, field):
        return pltpu.make_async_remote_copy(
            src_ref=field.at[4 - 3 * core, TOP : TOP + NY], dst_ref=field.at[5 * core, TOP : TOP + NY],
            send_sem=hs_sem.at[k, 0], recv_sem=hr_sem.at[k, 0], device_id=(mate,), device_id_type=MESH,
        )

    def far_coarse(k):
        return pltpu.make_async_remote_copy(
            src_ref=CP.at[k], dst_ref=NBC.at[k, 1 - core],
            send_sem=cps_sem.at[k, 1], recv_sem=cpr_sem.at[k, 1], device_id=(far,), device_id_type=MESH,
        )

    def mate_coarse(k):
        return pltpu.make_async_remote_copy(
            src_ref=CP.at[k], dst_ref=NBC.at[k, core],
            send_sem=cps_sem.at[k, 0], recv_sem=cpr_sem.at[k, 0], device_id=(mate,), device_id_type=MESH,
        )

    def clear(field):
        zero = jnp.zeros((TOP, NZ), F32)
        for x in range(6):
            field[x, 0:TOP] = zero
            field[x, TOP + NY :] = zero

        @pl.when(jnp.logical_not(has_far))
        def _():
            field[5 * core, TOP : TOP + NY] = jnp.zeros((NY, NZ), F32)

    def local_pair(first, second, src, field):
        for at, x in ((0, first), (NY, second)):
            high, low = split(src[x])
            XB[at : at + NY, 0:NZ] = high
            XB[at : at + NY, NZ:] = low
        high = XB[:, 0:NZ]
        low = XB[:, NZ:]
        out = dot(high, MH[...]) + dot(low, MH[...]) + dot(high, ML[...])
        field[first + 1, TOP : TOP + NY] = out[:NY]
        field[second + 1, TOP : TOP + NY] = out[NY:]

    def operator(field, out):
        for y in range(0, NY, 16):
            layer_sum = jnp.zeros((16, NZ), F32)
            lo = TOP + y
            for x in range(CX):
                c = field[x + 1, lo : lo + 16]
                up = field[x + 2, lo : lo + 16]
                dn = field[x, lo : lo + 16]
                beside = field[x + 1, lo + 1 : lo + 17] + field[x + 1, lo - 1 : lo + 15] + neighbours_z(c)
                value = (6.0 + SG[x, y : y + 16]) * c - (up + dn + beside) + WD[x, y : y + 16] * (up - dn)
                out[x, y : y + 16] = value
                layer_sum = layer_sum + value
            SUM[y : y + 16] = layer_sum

    def coarse_start(k):
        pass

    def expand(own, low, high):
        cx3 = jnp.concatenate([masked(own), masked(low), masked(high)], axis=1)
        ch, cl = split(cx3)
        e = dot3((BYH[...], BYL[...]), (ch, cl))
        e2 = dot3((BY2H[...], BY2L[...]), (ch[:, :128], cl[:, :128]))
        rows = jnp.concatenate([e[:, 0:128], e[:, 128:256], e[:, 256:384]], axis=0)
        rh, rl = split(rows)
        S3[...] = dot3((rh, rl), (BZH[...], BZL[...]))
        eh, el = split(e2)
        G0[...] = dot3((eh, el), (BZH[...], BZL[...])) - dot3((rh[:NY], rl[:NY]), (TBH[...], TBL[...]))

    def spread_terms(x, y):
        s = S3[y : y + 16]
        sg = SG[x, y : y + 16]
        g = G0[y : y + 16]
        if x == 0:
            w0 = WD[0, y : y + 16]
            return g + (sg - 1.0 + w0) * s - (1.0 + w0) * S3[NY + y : NY + y + 16]
        if x == CX - 1:
            w3 = WD[CX - 1, y : y + 16]
            return g + (sg - 1.0 - w3) * s - (1.0 - w3) * S3[2 * NY + y : 2 * NY + y + 16]
        return g + (sg - 2.0) * s

    def coarse_finish(k):
        own, other, every = axis_sums(k, 2, ALLR)
        far_y = far // 32
        same = (far_y // 2) == (cy // 2)
        top = GP[6] * every[:PK]
        mine = CP[k] + GP[5] * own[:PK] + top
        mate_part = NBC[k, 1 - core] + GP[5] * own[:PK] + top
        far_part = NBC[k, core] + GP[5] * jnp.where(same, own[:PK], other[:PK]) + top
        far_part = jnp.where(has_far, far_part, 0.0)
        low = jnp.where(core == 0, far_part, mate_part)
        high = jnp.where(core == 0, mate_part, far_part)
        return mine, low, high, every

    def wait_coarse_neighbours(k):
        mate_coarse(k).wait_recv()

        @pl.when(has_far)
        def _():
            far_coarse(k).wait_recv()

    step = to_mate(0, ALLR)
    loads[3].wait()
    for y in range(0, NZ, 64):
        MH[y : y + 64], ML[y : y + 64] = split(MI[y : y + 64])
    loads[4].wait()
    for level in range(LEVELS):
        g = GM[level] * (1.0 / (CX * 2 ** (level + 1)) ** 0.5)
        GP[level] = jnp.concatenate([g[:PK], g[PK:]], axis=1)
    step.wait_recv()
    SND[0, 1] = SND[0, 0] + RCV[0, 0]
    CP[0] = GP[0] * SND[0, 1, :PK]
    steps = to_axis(0, 0, ALLR)
    local_pair(0, 3, R, L)
    edges(0, L)
    for c in steps:
        c.wait_recv()
    own, other, every = axis_sums(0, 0, ALLR)
    SND[0, 2] = every
    steps = to_axis(0, 1, ALLR)
    CP[0] += GP[1] * own[:PK] + GP[2] * every[:PK]
    local_pair(1, 2, R, L)
    clear(L)
    for c in steps:
        c.wait_recv()
    own, other, every = axis_sums(0, 1, ALLR)
    SND[0, 3] = every
    steps = to_axis(0, 2, ALLR)
    CP[0] += GP[3] * own[:PK] + GP[4] * every[:PK]
    mate_coarse(0).start()

    @pl.when(has_far)
    def _():
        far_coarse(0).start()

    bzt = bz2.T
    BZH[...], BZL[...] = split(bzt)
    TBH[...], TBL[...] = split(neighbours_z(bzt))
    BYH[...], BYL[...] = split(by)
    zero = jnp.zeros((1, KY), F32)
    by2 = 6.0 * by - jnp.concatenate([by[1:], zero], axis=0) - jnp.concatenate([zero, by[:-1]], axis=0)
    BY2H[...], BY2L[...] = split(by2)
    loads[5].wait()
    loads[6].wait()
    for y in range(0, NY, 16):
        ssum = SG[0, y : y + 16] + SG[1, y : y + 16] + SG[2, y : y + 16] + SG[3, y : y + 16]
        CS[y : y + 16] = ssum + WD[0, y : y + 16] - WD[3, y : y + 16] - 6.0

    mate_edge(0, L).wait_recv()

    @pl.when(has_far)
    def _():
        edge_copy(0, L).wait_recv()

    operator(L, AL)
    PL[...] = project(SUM[...])
    for c in steps:
        c.wait_recv()
    wait_coarse_neighbours(0)
    mine, low, high, every = coarse_finish(0)
    rr = total(every[PK:])
    expand(mine, low, high)
    for y in range(0, NY, 16):
        s = S3[y : y + 16]
        w0 = WD[0, y : y + 16]
        w3 = WD[3, y : y + 16]
        X[y : y + 16] = (
            4.0 * G0[y : y + 16] + CS[y : y + 16] * s
            - (1.0 + w0) * S3[NY + y : NY + y + 16] - (1.0 - w3) * S3[2 * NY + y : 2 * NY + y + 16]
        )
    SND[1, 0, :PK] = PL[...] + project(X[...])

    step = to_mate(1, PKR)
    beta = jnp.sqrt(rr)
    inv = 1.0 / beta

    def build_w(x):
        for y in range(0, NY, 16):
            W[x, y : y + 16] = (AL[x, y : y + 16] + spread_terms(x, y)) * inv

    build_w(0)
    build_w(3)
    step.wait_recv()
    SND[1, 1, :PK] = SND[1, 0, :PK] + RCV[1, 0, :PK]
    CP[1] = GP[0] * SND[1, 1, :PK]
    steps = to_axis(1, 0, PKR)
    local_pair(0, 3, W, LW)
    edges(1, LW)
    build_w(1)
    build_w(2)
    for c in steps:
        c.wait_recv()
    own, other, every = axis_sums(1, 0, PKR)
    SND[1, 2, :PK] = every
    steps = to_axis(1, 1, PKR)
    CP[1] += GP[1] * own + GP[2] * every
    local_pair(1, 2, W, LW)
    clear(LW)
    for c in steps:
        c.wait_recv()
    own, other, every = axis_sums(1, 1, PKR)
    SND[1, 3, :PK] = every
    steps = to_axis(1, 2, PKR)
    CP[1] += GP[3] * own + GP[4] * every
    mate_coarse(1).start()

    @pl.when(has_far)
    def _():
        far_coarse(1).start()

    for x in range(CX):
        for y in range(0, NY, 16):
            Z1[x, y : y + 16] = (L[x + 1, TOP + y : TOP + y + 16] + S3[y : y + 16]) * inv
    vw = jnp.zeros((8, NZ), F32)
    ww = jnp.zeros((8, NZ), F32)
    for x in range(CX):
        for y in range(0, NY, 16):
            w = W[x, y : y + 16]
            vw = vw + fold(R[x, y : y + 16] * w)
            ww = ww + fold(w * w)
    vw = fold_lanes(vw) * inv
    ww = fold_lanes(ww)

    mate_edge(1, LW).wait_recv()

    @pl.when(has_far)
    def _():
        edge_copy(1, LW).wait_recv()

    operator(LW, Q)
    for c in steps:
        c.wait_recv()
    wait_coarse_neighbours(1)
    mine, low, high, _every = coarse_finish(1)
    expand(mine * inv, low * inv, high * inv)
    vq = jnp.zeros((8, NZ), F32)
    wq = jnp.zeros((8, NZ), F32)
    qq = jnp.zeros((8, NZ), F32)
    for x in range(CX):
        for y in range(0, NY, 16):
            q = Q[x, y : y + 16] + spread_terms(x, y)
            Q[x, y : y + 16] = q
            vq = vq + fold(R[x, y : y + 16] * q)
            wq = wq + fold(W[x, y : y + 16] * q)
            qq = qq + fold(q * q)
    row = lax.broadcasted_iota(jnp.int32, (8, 128), 0)
    parts = jnp.zeros((8, 128), F32)
    for i, part in enumerate((vw, ww, fold_lanes(vq) * inv, fold_lanes(wq), fold_lanes(qq))):
        parts = jnp.where(row == i, jnp.sum(part, axis=0, keepdims=True), parts)
    SC[0] = parts

    SND[2, 0, PK:] = parts
    step = to_mate(2, SCR)
    for x in range(CX):
        for y in range(0, NY, 16):
            U2[x, y : y + 16] = LW[x + 1, TOP + y : TOP + y + 16] + S3[y : y + 16]
    step.wait_recv()
    SND[2, 1, PK:] = SND[2, 0, PK:] + RCV[2, 0, PK:]
    for axis in range(3):
        for c in to_axis(2, axis, SCR):
            c.wait_recv()
        _own, _other, every = axis_sums(2, axis, SCR)
        if axis < 2:
            SND[2, 2 + axis, PK:] = every
    sums = jnp.sum(every, axis=1, keepdims=True)
    h11, gww, gvq, gwq, gqq = [sums[i : i + 1] for i in range(5)]
    rho = gwq / gww
    qhat = gqq / gww
    scale = beta / gww / (qhat - rho * rho)
    one = scale * (qhat * h11 - rho * gvq)
    two = scale * (gvq - rho * h11)
    for x in range(CX):
        for y in range(0, NY, 16):
            sol[x, y : y + 16] = one * Z1[x, y : y + 16] + two * U2[x, y : y + 16]
            res[x, y : y + 16] = R[x, y : y + 16] - one * W[x, y : y + 16] - two * Q[x, y : y + 16]

    for c in sends:
        c.wait_send()
    for k in range(2):
        mate_coarse(k).wait_send()

    @pl.when(has_far)
    def _():
        for k in range(2):
            far_coarse(k).wait_send()
        edge_copy(0, L).wait_send()
        edge_copy(1, LW).wait_send()


def on_device(right_side, sigma, wind, local_inverse, basis_y, basis_z, gamma):
    field = jax.ShapeDtypeStruct((CX, NY, NZ), F32)
    v = pltpu.VMEM
    dma = pltpu.SemaphoreType.DMA
    block = (CX, NY, NZ)
    return pl.pallas_call(
        kernel,
        out_shape=(field, field),
        in_specs=[pl.BlockSpec(memory_space=pl.ANY)] * 7,
        out_specs=[pl.BlockSpec(memory_space=pltpu.VMEM)] * 2,
        scratch_shapes=[
            v(block, F32), v(block, F32), v(block, F32), v((NZ, NZ), F32), v((NY, KY), F32), v((NZ, KZ), F32),
            v((LEVELS, KY, KZ), F32),
            v((2 * NY, 2 * NZ), BF16), v((NZ, NZ), BF16), v((NZ, NZ), BF16),
            v((6, PADY, NZ), F32), v((6, PADY, NZ), F32), v(block, F32), v(block, F32), v(block, F32), v(block, F32),
            v(block, F32),
            v((128, NZ), BF16), v((128, NZ), BF16), v((128, NZ), BF16), v((128, NZ), BF16),
            v((NZ, 128), BF16), v((NZ, 128), BF16),
            v((NY, KY), BF16), v((NY, KY), BF16), v((NY, KY), BF16), v((NY, KY), BF16),
            v((KY, NY), BF16), v((KY, NY), BF16), v((LEVELS, PK, 128), F32),
            v((3 * NY, NZ), F32), v((NY, NZ), F32), v((NY, NZ), F32), v((NY, NZ), F32), v((NY, NZ), F32),
            v((PK, 128), F32),
            v((3, 4, PAY, 128), F32), v((3, 10, PAY, 128), F32), v((2, PK, 128), F32), v((2, 2, PK, 128), F32),
            v((1, 8, 128), F32),
            dma((7,)), dma((3, 10)), dma((3, 10)), dma((2, 2)), dma((2, 2)), dma((2, 2)), dma((2, 2)),
        ],
        compiler_params=pltpu.CompilerParams(
            collective_id=0, has_side_effects=True, vmem_limit_bytes=48 * 1024 * 1024
        ),
    )(right_side, sigma, wind, local_inverse, basis_y, basis_z, gamma)


def solution(mesh):
    row = P("sub", None, None)
    in_specs = (row, row, row, row, P(), P(), P())
    return jax.shard_map(on_device, mesh=mesh, in_specs=in_specs, out_specs=(row, row), check_vma=False)
```

```python
import functools

import jax
import jax.numpy as jnp
from jax import lax
from jax.experimental import pallas as pl
from jax.experimental.pallas import tpu as pltpu
from jax.sharding import PartitionSpec as P

MESH = pl.DeviceIdType.MESH
F32 = jnp.float32
BF16 = jnp.bfloat16

CX, NY, NZ, KY, KZ, LEVELS = 4, 128, 512, 32, 64, 7
PK = 16
PAY = PK + 8
TOP = 8
PADY = NY + 2 * TOP


def split(x):
    high = x.astype(BF16)
    return high, (x - high.astype(F32)).astype(BF16)


def dot(a, b):
    return jnp.dot(a, b, preferred_element_type=F32)


def dot3(a, b):
    ah, al = a
    bh, bl = b
    return dot(ah, bh) + dot(al, bh) + dot(ah, bl)


def lanes(shape):
    return lax.broadcasted_iota(jnp.int32, shape, len(shape) - 1)


def pack(c):
    return jnp.where(lanes((PK, 128)) < KZ, c[:PK], c[PK:])


def masked(c):
    low = lanes((PK, 128)) < KZ
    return jnp.concatenate([jnp.where(low, c, 0.0), jnp.where(low, 0.0, c)], axis=0)


def neighbours_z(c):
    lane = lanes(c.shape)
    ahead = jnp.where(lane == NZ - 1, 0.0, pltpu.roll(c, NZ - 1, 1))
    behind = jnp.where(lane == 0, 0.0, pltpu.roll(c, 1, 1))
    return ahead + behind


def total(x):
    return jnp.sum(jnp.sum(x, axis=0, keepdims=True), axis=1, keepdims=True)


def fold(x):
    acc = x[0:8]
    for i in range(8, x.shape[0], 8):
        acc = acc + x[i : i + 8]
    return acc


def fold_lanes(x):
    return x[:, 0:128] + x[:, 128:256] + x[:, 256:384] + x[:, 384:512]


def kernel(
    r_h, sg_h, wd_h, mi_h, by_h, bz_h, gm_h,
    R, W, Q, Z1, U2, AB,
    SG, WD, MI, BY, BZ, GM,
    XB, MH, ML, L, LW, AL,
    BZH, BZL, TBH, TBL, B2H, B2L, BYH, BYL, BY2H, BY2L, BTH, BTL, GP,
    S3, G0, X, CS, SUM, PL,
    SND, RCV, CP, NBC,
    ld_sem, snd_sem, rcv_sem, cps_sem, cpr_sem, hs_sem, hr_sem,
):
    b = lax.axis_index("sub")
    core = lax.rem(b, 2)
    cx = lax.rem(b // 2, 4)
    cz = lax.rem(b // 8, 4)
    cy = b // 32
    coords = (cx, cz, cy)
    strides = (2, 8, 32)
    mate = b + 1 - 2 * core
    far = b - 1 + 2 * core
    has_far = jnp.logical_and(far >= 0, far < 128)

    def peer(axis, d):
        c = coords[axis]
        return b + (lax.rem(c + d, 4) - c) * strides[axis]

    loads = [
        pltpu.make_async_copy(src, dst, ld_sem.at[i])
        for i, (src, dst) in enumerate(
            [(r_h, R), (by_h, BY), (bz_h, BZ), (mi_h.at[0], MI), (gm_h, GM), (sg_h, SG), (wd_h, WD)]
        )
    ]
    for c in loads:
        c.start()

    barrier = pltpu.get_barrier_semaphore()
    peers = [mate] + [peer(a, d) for a in range(3) for d in (1, 2, 3)]
    for p in peers:
        pl.semaphore_signal(barrier, inc=1, device_id=(p,), device_id_type=MESH)

    @pl.when(has_far)
    def _():
        pl.semaphore_signal(barrier, inc=1, device_id=(far,), device_id_type=MESH)

    loads[1].wait()
    loads[2].wait()
    by_t = BY[...]
    bz = BZ[...]
    bzt = jnp.concatenate([bz, bz], axis=0)
    B2H[...], B2L[...] = split(bzt.T)
    BTH[...], BTL[...] = split(by_t)

    def project(field):
        half = dot3(split(field), (B2H[...], B2L[...]))
        return pack(dot3((BTH[...], BTL[...]), split(half)))

    loads[0].wait()
    acc = jnp.zeros((8, NZ), F32)
    for y in range(0, NY, 16):
        s = jnp.zeros((16, NZ), F32)
        q = jnp.zeros((16, NZ), F32)
        for x in range(CX):
            v = R[x, y : y + 16]
            s = s + v
            q = q + v * v
        X[y : y + 16] = s
        acc = acc + fold(q)
    SND[0, 0, :PK] = project(X[...])
    SND[0, 0, PK:] = fold_lanes(acc)

    pl.semaphore_wait(barrier, len(peers) + has_far.astype(jnp.int32))

    sends = []

    def send(src, dst, ss, rs, device):
        c = pltpu.make_async_remote_copy(
            src_ref=src, dst_ref=dst, send_sem=ss, recv_sem=rs, device_id=(device,), device_id_type=MESH
        )
        c.start()
        return c

    def to_mate(k, rows):
        c = send(SND.at[k, 0, rows], RCV.at[k, 0, rows], snd_sem.at[k, 0], rcv_sem.at[k, 0], mate)
        sends.append(c)
        return c

    def to_axis(k, axis, rows):
        cs = []
        for d in (1, 2, 3):
            i = 1 + 3 * axis + d - 1
            cs.append(
                send(SND.at[k, 1 + axis, rows], RCV.at[k, i, rows], snd_sem.at[k, i], rcv_sem.at[k, i], peer(axis, d))
            )
        sends.extend(cs)
        return cs

    def axis_sums(k, axis, rows):
        base = 1 + 3 * axis
        odd = lax.rem(coords[axis], 2)
        own = SND[k, 1 + axis, rows] + RCV[k, base + 2 - 2 * odd, rows]
        other = RCV[k, base + 1, rows] + RCV[k, base + 2 * odd, rows]
        return own, other, own + other

    ALLR = pl.ds(0, PAY)
    PKR = pl.ds(0, PK)
    SCR = pl.ds(PK, 8)

    def edges(k, field):
        send_mate = send(
            field.at[4 - 3 * core, TOP : TOP + NY], field.at[5 * core, TOP : TOP + NY],
            hs_sem.at[k, 0], hr_sem.at[k, 0], mate,
        )
        sends.append(send_mate)

        @pl.when(has_far)
        def _():
            send(
                field.at[1 + 3 * core, TOP : TOP + NY], field.at[5 - 5 * core, TOP : TOP + NY],
                hs_sem.at[k, 1], hr_sem.at[k, 1], far,
            )

    def edge_copy(k, field):
        return pltpu.make_async_remote_copy(
            src_ref=field.at[1 + 3 * core, TOP : TOP + NY], dst_ref=field.at[5 - 5 * core, TOP : TOP + NY],
            send_sem=hs_sem.at[k, 1], recv_sem=hr_sem.at[k, 1], device_id=(far,), device_id_type=MESH,
        )

    def mate_edge(k, field):
        return pltpu.make_async_remote_copy(
            src_ref=field.at[4 - 3 * core, TOP : TOP + NY], dst_ref=field.at[5 * core, TOP : TOP + NY],
            send_sem=hs_sem.at[k, 0], recv_sem=hr_sem.at[k, 0], device_id=(mate,), device_id_type=MESH,
        )

    def far_coarse(k):
        return pltpu.make_async_remote_copy(
            src_ref=CP.at[k], dst_ref=NBC.at[k, 1 - core],
            send_sem=cps_sem.at[k, 1], recv_sem=cpr_sem.at[k, 1], device_id=(far,), device_id_type=MESH,
        )

    def mate_coarse(k):
        return pltpu.make_async_remote_copy(
            src_ref=CP.at[k], dst_ref=NBC.at[k, core],
            send_sem=cps_sem.at[k, 0], recv_sem=cpr_sem.at[k, 0], device_id=(mate,), device_id_type=MESH,
        )

    def clear(field):
        zero = jnp.zeros((TOP, NZ), F32)
        for x in range(6):
            field[x, 0:TOP] = zero
            field[x, TOP + NY :] = zero

        @pl.when(jnp.logical_not(has_far))
        def _():
            field[5 * core, TOP : TOP + NY] = jnp.zeros((NY, NZ), F32)

    def local_pair(first, second, src, field):
        for at, x in ((0, first), (NY, second)):
            high, low = split(src[x])
            XB[at : at + NY, 0:NZ] = high
            XB[at : at + NY, NZ:] = low
        high = XB[:, 0:NZ]
        low = XB[:, NZ:]
        out = dot(high, MH[...]) + dot(low, MH[...]) + dot(high, ML[...])
        field[first + 1, TOP : TOP + NY] = out[:NY]
        field[second + 1, TOP : TOP + NY] = out[NY:]

    def operator(field, out):
        for y in range(0, NY, 16):
            layer_sum = jnp.zeros((16, NZ), F32)
            lo = TOP + y
            for x in range(CX):
                c = field[x + 1, lo : lo + 16]
                up = field[x + 2, lo : lo + 16]
                dn = field[x, lo : lo + 16]
                beside = field[x + 1, lo + 1 : lo + 17] + field[x + 1, lo - 1 : lo + 15] + neighbours_z(c)
                value = (6.0 + SG[x, y : y + 16]) * c - (up + dn + beside) + WD[x, y : y + 16] * (up - dn)
                out[x, y : y + 16] = value
                layer_sum = layer_sum + value
            SUM[y : y + 16] = layer_sum

    def expand(own, low, high):
        cx3 = jnp.concatenate([masked(own), masked(low), masked(high)], axis=1)
        ch, cl = split(cx3)
        e = dot3((BYH[...], BYL[...]), (ch, cl))
        e2 = dot3((BY2H[...], BY2L[...]), (ch[:, :128], cl[:, :128]))
        rows = jnp.concatenate([e[:, 0:128], e[:, 128:256], e[:, 256:384]], axis=0)
        rh, rl = split(rows)
        S3[...] = dot3((rh, rl), (BZH[...], BZL[...]))
        eh, el = split(e2)
        G0[...] = dot3((eh, el), (BZH[...], BZL[...])) - dot3((rh[:NY], rl[:NY]), (TBH[...], TBL[...]))

    def spread_terms(x, y):
        s = S3[y : y + 16]
        sg = SG[x, y : y + 16]
        g = G0[y : y + 16]
        if x == 0:
            w0 = WD[0, y : y + 16]
            return g + (sg - 1.0 + w0) * s - (1.0 + w0) * S3[NY + y : NY + y + 16]
        if x == CX - 1:
            w3 = WD[CX - 1, y : y + 16]
            return g + (sg - 1.0 - w3) * s - (1.0 - w3) * S3[2 * NY + y : 2 * NY + y + 16]
        return g + (sg - 2.0) * s

    def coarse_finish(k):
        own, other, every = axis_sums(k, 2, ALLR)
        far_y = far // 32
        same = (far_y // 2) == (cy // 2)
        top = GP[6] * every[:PK]
        mine = CP[k] + GP[5] * own[:PK] + top
        mate_part = NBC[k, 1 - core] + GP[5] * own[:PK] + top
        far_part = NBC[k, core] + GP[5] * jnp.where(same, own[:PK], other[:PK]) + top
        far_part = jnp.where(has_far, far_part, 0.0)
        low = jnp.where(core == 0, far_part, mate_part)
        high = jnp.where(core == 0, mate_part, far_part)
        return mine, low, high, every

    def wait_coarse_neighbours(k):
        mate_coarse(k).wait_recv()

        @pl.when(has_far)
        def _():
            far_coarse(k).wait_recv()

    step = to_mate(0, ALLR)
    loads[3].wait()
    for y in range(0, NZ, 64):
        MH[y : y + 64], ML[y : y + 64] = split(MI[y : y + 64])
    loads[4].wait()
    for level in range(LEVELS):
        g = GM[level] * (1.0 / (CX * 2 ** (level + 1)) ** 0.5)
        GP[level] = jnp.concatenate([g[:PK], g[PK:]], axis=1)
    step.wait_recv()
    SND[0, 1] = SND[0, 0] + RCV[0, 0]
    CP[0] = GP[0] * SND[0, 1, :PK]
    steps = to_axis(0, 0, ALLR)
    local_pair(0, 3, R, L)
    edges(0, L)
    for c in steps:
        c.wait_recv()
    own, other, every = axis_sums(0, 0, ALLR)
    SND[0, 2] = every
    steps = to_axis(0, 1, ALLR)
    CP[0] += GP[1] * own[:PK] + GP[2] * every[:PK]
    local_pair(1, 2, R, L)
    clear(L)
    for c in steps:
        c.wait_recv()
    own, other, every = axis_sums(0, 1, ALLR)
    SND[0, 3] = every
    steps = to_axis(0, 2, ALLR)
    CP[0] += GP[3] * own[:PK] + GP[4] * every[:PK]
    mate_coarse(0).start()

    @pl.when(has_far)
    def _():
        far_coarse(0).start()

    by = by_t.T
    BZH[...], BZL[...] = split(bzt)
    TBH[...], TBL[...] = split(neighbours_z(bzt))
    BYH[...], BYL[...] = split(by)
    zero = jnp.zeros((1, KY), F32)
    by2 = 6.0 * by - jnp.concatenate([by[1:], zero], axis=0) - jnp.concatenate([zero, by[:-1]], axis=0)
    BY2H[...], BY2L[...] = split(by2)
    loads[5].wait()
    loads[6].wait()
    for y in range(0, NY, 16):
        ssum = SG[0, y : y + 16] + SG[1, y : y + 16] + SG[2, y : y + 16] + SG[3, y : y + 16]
        CS[y : y + 16] = ssum + WD[0, y : y + 16] - WD[3, y : y + 16] - 6.0

    mate_edge(0, L).wait_recv()

    @pl.when(has_far)
    def _():
        edge_copy(0, L).wait_recv()

    operator(L, AL)
    PL[...] = project(SUM[...])
    for c in steps:
        c.wait_recv()
    wait_coarse_neighbours(0)
    mine, low, high, every = coarse_finish(0)
    rr = total(every[PK:])
    expand(mine, low, high)
    for y in range(0, NY, 16):
        s = S3[y : y + 16]
        w0 = WD[0, y : y + 16]
        w3 = WD[3, y : y + 16]
        X[y : y + 16] = (
            4.0 * G0[y : y + 16] + CS[y : y + 16] * s
            - (1.0 + w0) * S3[NY + y : NY + y + 16] - (1.0 - w3) * S3[2 * NY + y : 2 * NY + y + 16]
        )
    SND[1, 0, :PK] = PL[...] + project(X[...])

    step = to_mate(1, PKR)
    beta = jnp.sqrt(rr)
    inv = 1.0 / beta

    def build_w(x):
        for y in range(0, NY, 16):
            W[x, y : y + 16] = (AL[x, y : y + 16] + spread_terms(x, y)) * inv

    build_w(0)
    build_w(3)
    step.wait_recv()
    SND[1, 1, :PK] = SND[1, 0, :PK] + RCV[1, 0, :PK]
    CP[1] = GP[0] * SND[1, 1, :PK]
    steps = to_axis(1, 0, PKR)
    local_pair(0, 3, W, LW)
    edges(1, LW)
    build_w(1)
    build_w(2)
    for c in steps:
        c.wait_recv()
    own, other, every = axis_sums(1, 0, PKR)
    SND[1, 2, :PK] = every
    steps = to_axis(1, 1, PKR)
    CP[1] += GP[1] * own + GP[2] * every
    local_pair(1, 2, W, LW)
    clear(LW)
    for c in steps:
        c.wait_recv()
    own, other, every = axis_sums(1, 1, PKR)
    SND[1, 3, :PK] = every
    steps = to_axis(1, 2, PKR)
    CP[1] += GP[3] * own + GP[4] * every
    mate_coarse(1).start()

    @pl.when(has_far)
    def _():
        far_coarse(1).start()

    for x in range(CX):
        for y in range(0, NY, 16):
            Z1[x, y : y + 16] = (L[x + 1, TOP + y : TOP + y + 16] + S3[y : y + 16]) * inv
    vw = jnp.zeros((8, NZ), F32)
    ww = jnp.zeros((8, NZ), F32)
    for x in range(CX):
        for y in range(0, NY, 16):
            w = W[x, y : y + 16]
            vw = vw + fold(R[x, y : y + 16] * w)
            ww = ww + fold(w * w)
    vw = fold_lanes(vw) * inv
    ww = fold_lanes(ww)

    mate_edge(1, LW).wait_recv()

    @pl.when(has_far)
    def _():
        edge_copy(1, LW).wait_recv()

    operator(LW, Q)
    for c in steps:
        c.wait_recv()
    wait_coarse_neighbours(1)
    mine, low, high, _every = coarse_finish(1)
    expand(mine * inv, low * inv, high * inv)
    vq = jnp.zeros((8, NZ), F32)
    wq = jnp.zeros((8, NZ), F32)
    qq = jnp.zeros((8, NZ), F32)
    for x in range(CX):
        for y in range(0, NY, 16):
            q = Q[x, y : y + 16] + spread_terms(x, y)
            Q[x, y : y + 16] = q
            vq = vq + fold(R[x, y : y + 16] * q)
            wq = wq + fold(W[x, y : y + 16] * q)
            qq = qq + fold(q * q)
    row = lax.broadcasted_iota(jnp.int32, (8, 128), 0)
    parts = jnp.zeros((8, 128), F32)
    for i, part in enumerate((vw, ww, fold_lanes(vq) * inv, fold_lanes(wq), fold_lanes(qq))):
        parts = jnp.where(row == i, jnp.sum(part, axis=0, keepdims=True), parts)

    SND[2, 0, PK:] = parts
    step = to_mate(2, SCR)
    for x in range(CX):
        for y in range(0, NY, 16):
            U2[x, y : y + 16] = LW[x + 1, TOP + y : TOP + y + 16] + S3[y : y + 16]
    step.wait_recv()
    SND[2, 1, PK:] = SND[2, 0, PK:] + RCV[2, 0, PK:]
    for axis in range(3):
        for c in to_axis(2, axis, SCR):
            c.wait_recv()
        _own, _other, every = axis_sums(2, axis, SCR)
        if axis < 2:
            SND[2, 2 + axis, PK:] = every
    sums = jnp.sum(every, axis=1, keepdims=True)
    h11, gww, gvq, gwq, gqq = [sums[i : i + 1] for i in range(5)]
    rho = gwq / gww
    qhat = gqq / gww
    scale = beta / gww / (qhat - rho * rho)
    one = scale * (qhat * h11 - rho * gvq)
    two = scale * (gvq - rho * h11)
    AB[...] = jnp.where(row == 0, one, two)

    for c in sends:
        c.wait_send()
    for k in range(2):
        mate_coarse(k).wait_send()

    @pl.when(has_far)
    def _():
        for k in range(2):
            far_coarse(k).wait_send()
        edge_copy(0, L).wait_send()
        edge_copy(1, LW).wait_send()


def combine(R, W, Q, Z1, U2, AB, sol_h, res_h, SOL, RES, sem):
    one = AB[0:1, 0:1]
    two = AB[1:2, 0:1]
    copies = []
    for x in range(CX):
        for y in range(0, NY, 16):
            SOL[x, y : y + 16] = one * Z1[x, y : y + 16] + two * U2[x, y : y + 16]
            RES[x, y : y + 16] = R[x, y : y + 16] - one * W[x, y : y + 16] - two * Q[x, y : y + 16]
        for i, (src, dst) in enumerate(((SOL, sol_h), (RES, res_h))):
            c = pltpu.make_async_copy(src.at[x], dst.at[x], sem.at[2 * x + i])
            c.start()
            copies.append(c)
    for c in copies:
        c.wait()


def on_device(right_side, sigma, wind, local_inverse, basis_y, basis_z, gamma):
    field = jax.ShapeDtypeStruct((CX, NY, NZ), F32)
    v = pltpu.VMEM
    dma = pltpu.SemaphoreType.DMA
    block = (CX, NY, NZ)
    parts = pl.pallas_call(
        kernel,
        out_shape=(field,) * 5 + (jax.ShapeDtypeStruct((8, 128), F32),),
        in_specs=[pl.BlockSpec(memory_space=pltpu.HBM)] * 7,
        out_specs=[pl.BlockSpec(memory_space=pltpu.VMEM)] * 6,
        scratch_shapes=[
            v(block, F32), v(block, F32), v((NZ, NZ), F32), v((KY, NY), F32), v((KZ, NZ), F32),
            v((LEVELS, KY, KZ), F32),
            v((2 * NY, 2 * NZ), BF16), v((NZ, NZ), BF16), v((NZ, NZ), BF16),
            v((6, PADY, NZ), F32), v((6, PADY, NZ), F32), v(block, F32),
            v((128, NZ), BF16), v((128, NZ), BF16), v((128, NZ), BF16), v((128, NZ), BF16),
            v((NZ, 128), BF16), v((NZ, 128), BF16),
            v((NY, KY), BF16), v((NY, KY), BF16), v((NY, KY), BF16), v((NY, KY), BF16),
            v((KY, NY), BF16), v((KY, NY), BF16), v((LEVELS, PK, 128), F32),
            v((3 * NY, NZ), F32), v((NY, NZ), F32), v((NY, NZ), F32), v((NY, NZ), F32), v((NY, NZ), F32),
            v((PK, 128), F32),
            v((3, 4, PAY, 128), F32), v((3, 10, PAY, 128), F32), v((2, PK, 128), F32), v((2, 2, PK, 128), F32),
            dma((7,)), dma((3, 10)), dma((3, 10)), dma((2, 2)), dma((2, 2)), dma((2, 2)), dma((2, 2)),
        ],
        compiler_params=pltpu.CompilerParams(
            collective_id=0, has_side_effects=True, vmem_limit_bytes=40 * 1024 * 1024
        ),
    )(*[pltpu.with_memory_space_constraint(t, pltpu.HBM) for t in (right_side, sigma, wind, local_inverse, basis_y.T, basis_z.T, gamma)])
    return pl.pallas_call(
        combine,
        out_shape=(field, field),
        in_specs=[pl.BlockSpec(memory_space=pltpu.VMEM)] * 6,
        out_specs=[pl.BlockSpec(memory_space=pltpu.HBM)] * 2,
        scratch_shapes=[v(block, F32), v(block, F32), dma((2 * CX,))],
        compiler_params=pltpu.CompilerParams(vmem_limit_bytes=16 * 1024 * 1024),
    )(*parts)


def solution(mesh):
    row = P("sub", None, None)
    in_specs = (row, row, row, row, P(), P(), P())
    return jax.shard_map(on_device, mesh=mesh, in_specs=in_specs, out_specs=(row, row), check_vma=False)
```
